32 devices in a mesh: row: 4 (over y, x), col: 8 (over z, core).
Axes of the slice: x: 2, y: 2, z: 4, core: 2. Of those that a mesh axis runs over, the one named last changes fastest.
Arguments:
- initial_field: float32 [256, 256, 256], P(('row', 'col')), may hold values from -5 to 5
Outputs:
- advanced_field: float32 [256, 256, 256], P(('row', 'col'))
The draws below stay inside these ranges and needn't reach their ends.
All inputs are finite; a program needn't handle non-finite values.
Results may differ from the reference program's by a relative error of at most 0.0003.
Values sent between devices are 32-bit elements; how exact they have to be, the bound alone decides.
A program may use at most 128 MiB of HBM per device.

```python
import math
import jax
import jax.numpy as jnp

NX = 256
NY = 256
NZ = 256


def level_of(stream_key, dims, split, least, high):
    def one(position, blocks):
        heights = jax.random.uniform(jax.random.fold_in(jax.random.fold_in(stream_key, 6), position), (blocks,), jnp.float32, least / len(split), high / len(split))
        return jnp.repeat(jnp.exp(heights), dims[position] // blocks).reshape((-1,) + (1,) * (len(dims) - position - 1))

    gain = one(*split[0])
    for cut in split[1:]:
        gain = gain * one(*cut)
    return gain


def noise(own_key, dims, scale, bound, split=(), dtype=jnp.bfloat16):
    result = scale * jax.random.normal(own_key, dims, jnp.float32)
    if split:
        result = result * level_of(own_key, dims, split, -0.22, 0.18)
    return jnp.clip(result, -bound, bound).astype(dtype)


def setup_inputs(seed: int = 0) -> dict:
    key_of = jax.random.split(jax.random.key(seed), 2)
    initial_field = noise(key_of[0], (NX, NY, NZ), 1.0, 5.0, ((0, 32),), jnp.float32)
    return dict(initial_field=initial_field)


growth_rate = 0.3
quadratic = 1.0
time_step = 0.2
wave_scale = 4.0


def wavenumbers(count, offset, length):
    indices = (offset + jnp.arange(count)).astype(jnp.int32)
    signed = jnp.where(indices * 2 < length, indices, indices - length)
    return wave_scale * signed.astype(jnp.float32) / length


def phi_values(argument):
    within = jnp.abs(argument) < 1.0
    inside = jnp.where(within, argument, 0.0)
    outside = jnp.where(within, 2.0, argument)
    series = []
    for degree in (1, 2, 3):
        running = jnp.zeros_like(argument) + 1.0 / math.factorial(11 + degree)
        for exponent in range(10, -1, -1):
            running = running * inside + 1.0 / math.factorial(exponent + degree)
        series.append(running)
    growth_term = jnp.exp(outside)
    closed_one = (growth_term - 1.0) / outside
    closed_two = (growth_term - 1.0 - outside) / (outside * outside)
    closed_three = (growth_term - 1.0 - outside - 0.5 * outside * outside) / (outside * outside * outside)
    return (jnp.where(within, series[0], closed_one), jnp.where(within, series[1], closed_two), jnp.where(within, series[2], closed_three))


def step_factors(ksq):
    lin = growth_rate - (1.0 - ksq) * (1.0 - ksq)
    scaled = time_step * lin
    half_phi, _, _ = phi_values(0.5 * scaled)
    first_phi, second_phi, third_phi = phi_values(scaled)
    e_half = jnp.exp(0.5 * scaled)
    q_half = 0.5 * time_step * half_phi
    e_full = jnp.exp(scaled)
    f_one = time_step * (first_phi - 3.0 * second_phi + 4.0 * third_phi)
    f_two = time_step * (second_phi - 2.0 * third_phi)
    f_three = time_step * (4.0 * third_phi - second_phi)
    return e_half, q_half, e_full, f_one, f_two, f_three


def reaction(values):
    return quadratic * values * values - values * values * values


def reference(initial_field):
    wave_x = wavenumbers(NX, 0, NX)
    wave_y = wavenumbers(NY, 0, NY)
    wave_z = wavenumbers(NZ, 0, NZ)
    ksq = wave_x[:, None, None] ** 2 + wave_y[None, :, None] ** 2 + wave_z[None, None, :] ** 2
    e_half, q_half, e_full, f_one, f_two, f_three = step_factors(ksq)

    def forward_fft(values):
        return jnp.fft.fftn(values)

    def inverse_fft(spectrum):
        return jnp.fft.ifftn(spectrum).real

    state_hat = forward_fft(initial_field)
    react_u = forward_fft(reaction(initial_field))
    first_hat = e_half * state_hat + q_half * react_u
    react_a = forward_fft(reaction(inverse_fft(first_hat)))
    second_hat = e_half * state_hat + q_half * react_a
    react_b = forward_fft(reaction(inverse_fft(second_hat)))
    third_hat = e_half * first_hat + q_half * (2.0 * react_b - react_u)
    react_c = forward_fft(reaction(inverse_fft(third_hat)))
    new_hat = e_full * state_hat + f_one * react_u + 2.0 * f_two * (react_a + react_b) + f_three * react_c
    return inverse_fft(new_hat).astype(jnp.float32)
```

```python
import functools
import math

import jax
import jax.numpy as jnp
import numpy as np
from jax import lax
from jax.experimental import pallas as pl
from jax.experimental.pallas import tpu as pltpu
from jax.sharding import PartitionSpec as P

growth_rate = 0.3
quadratic = 1.0
time_step = 0.2
wave_scale = 4.0


def wavenumbers(count, offset, length):
    indices = offset + jnp.arange(count)
    signed = jnp.where(indices * 2 < length, indices, indices - length)
    return wave_scale * signed.astype(jnp.float32) / length


def phi_values(argument):
    within = jnp.abs(argument) < 1.0
    inside = jnp.where(within, argument, 0.0)
    outside = jnp.where(within, 2.0, argument)
    series = []
    for degree in (1, 2, 3):
        running = jnp.zeros_like(argument) + 1.0 / math.factorial(11 + degree)
        for exponent in range(10, -1, -1):
            running = running * inside + 1.0 / math.factorial(exponent + degree)
        series.append(running)
    growth_term = jnp.exp(outside)
    closed_one = (growth_term - 1.0) / outside
    closed_two = (growth_term - 1.0 - outside) / (outside * outside)
    closed_three = (growth_term - 1.0 - outside - 0.5 * outside * outside) / (
        outside * outside * outside
    )
    return (
        jnp.where(within, series[0], closed_one),
        jnp.where(within, series[1], closed_two),
        jnp.where(within, series[2], closed_three),
    )


def step_factors(ksq):
    lin = growth_rate - (1.0 - ksq) * (1.0 - ksq)
    scaled = time_step * lin
    half_phi, _, _ = phi_values(0.5 * scaled)
    first_phi, second_phi, third_phi = phi_values(scaled)
    e_half = jnp.exp(0.5 * scaled)
    q_half = 0.5 * time_step * half_phi
    e_full = jnp.exp(scaled)
    f_one = time_step * (first_phi - 3.0 * second_phi + 4.0 * third_phi)
    f_two = time_step * (second_phi - 2.0 * third_phi)
    f_three = time_step * (4.0 * third_phi - second_phi)
    return (e_half, q_half, e_full, f_one, f_two, f_three)


def reaction(values):
    return quadratic * values * values - values * values * values


def cas_table(length):
    modes = jnp.arange(length, dtype=jnp.int32)
    product = jnp.mod(modes[:, None] * modes[None, :], length)
    angle = 2.0 * math.pi / length * product.astype(jnp.float32)
    return (jnp.cos(angle) + jnp.sin(angle)) / math.sqrt(length)


def contract(form, left, right):
    return jnp.einsum(
        form, left, right, precision=lax.Precision.HIGHEST, preferred_element_type=jnp.float32
    )


def move(blocks):
    return lax.all_to_all(blocks, ("row", "col"), split_axis=0, concat_axis=0, tiled=True)


def plain_body(initial_field):
    devices_all = lax.axis_size("row") * lax.axis_size("col")
    rows_x, size_y, size_z = initial_field.shape
    size_x = rows_x * devices_all
    share_y = size_y // devices_all
    table_z = cas_table(size_z)
    table_y = cas_table(size_y).reshape((devices_all, share_y, size_y))
    table_x = cas_table(size_x).reshape((devices_all, rows_x, size_x))
    offset = lax.axis_index(("row", "col")) * share_y
    wave_y = wavenumbers(share_y, offset, size_y)
    wave_z = wavenumbers(size_z, 0, size_z)
    wave_x = wavenumbers(size_x, 0, size_x)
    ksq = wave_y[:, None, None] ** 2 + wave_z[None, None, :] ** 2 + wave_x[None, :, None] ** 2
    e_half, q_half, e_full, f_one, f_two, f_three = step_factors(ksq)

    def forward_all(values):
        over_z = contract("xyn,nk->xyk", values, table_z)
        over_y = contract("sly,xyk->slxk", table_y, over_z)
        return contract("sxX,slxk->lXk", table_x, move(over_y))

    def inverse_all(spectra):
        over_x = contract("sxX,lXk->slxk", table_x, spectra)
        over_y = contract("slxk,sly->xyk", move(over_x), table_y)
        return contract("xyk,kn->xyn", over_y, table_z)

    def react_spectrum(spectrum):
        return forward_all(reaction(inverse_all(spectrum)))

    state_hat = forward_all(initial_field)
    react_u = forward_all(reaction(initial_field))
    first_hat = e_half * state_hat + q_half * react_u
    react_a = react_spectrum(first_hat)
    second_hat = e_half * state_hat + q_half * react_a
    react_b = react_spectrum(second_hat)
    third_hat = e_half * first_hat + q_half * (2.0 * react_b - react_u)
    react_c = react_spectrum(third_hat)
    new_hat = (
        e_full * state_hat + f_one * react_u + 2.0 * f_two * (react_a + react_b) + f_three * react_c
    )
    return inverse_all(new_hat)


LANES = 128
CORES = 2
LAYERS = 4
ROWS = 8


def split_table(length):
    modes = np.arange(length)
    angle = 2.0 * np.pi / length * ((modes[:, None] * modes[None, :]) % length)
    table = ((np.cos(angle) + np.sin(angle)) / np.sqrt(length)).astype(np.float32)
    upper = table.astype(jnp.bfloat16)
    lower = (table - upper.astype(np.float32)).astype(jnp.bfloat16)
    return upper, lower


def split_values(values):
    upper = values.astype(jnp.bfloat16)
    lower = (values - upper.astype(jnp.float32)).astype(jnp.bfloat16)
    return upper, lower


def kernel(
    count, columns, rows_x, share_y, size_x, size_y, size_z,
    field_in, left, right, out_to,
    send_f, got_f, send_i, got_i, held, third, total, q_half, f_two, f_three, field,
    came_f, twin_f, sent_f, passed_f, came_i, near_i, twin_i, sent_i, passed_i,
    swapped, swap_sent, plane_in, plane_out,
):
    row, col = lax.axis_index("row"), lax.axis_index("col")
    me = row * columns + col
    layer, core = col // CORES, col % CORES
    groups = count // LAYERS
    my_group = row * CORES + core
    middle = jnp.logical_and(layer > 0, layer < LAYERS - 1)
    units = jnp.where(middle, 2, 1)
    home = jnp.where(middle, layer - 1, 0)
    outer = jnp.where(layer < LAYERS // 2, 0, LAYERS - 1)
    near = jnp.where(layer < LAYERS // 2, 1, LAYERS - 2)
    twin = row * columns + (LAYERS - 1 - layer) * CORES + core
    block = rows_x * share_y
    halves = size_z // LANES
    pairs = share_y // 2
    parts = rows_x
    early = parts // 2
    chunks = 4
    chunk = block // chunks
    e_half = third

    def target(device):
        return dict(
            device_id=(device // columns, device % columns), device_id_type=pl.DeviceIdType.MESH
        )

    def unit_at(slot):
        return row * columns + jnp.where(middle, slot + 1, layer) * CORES + core

    def mul_left(values):
        upper, lower = split_values(values)
        stacked = jnp.concatenate([upper, lower, upper], axis=0)
        return jnp.dot(left[...], stacked, preferred_element_type=jnp.float32)

    def mul_right(values):
        upper, lower = split_values(values)
        stacked = jnp.concatenate([upper, lower, upper], axis=1)
        return jnp.dot(stacked, right[...], preferred_element_type=jnp.float32)

    def load(m):
        return pltpu.make_async_copy(field_in.at[m], field.at[home, m], plane_in.at[m])

    def store(m):
        return pltpu.make_async_copy(field.at[0, m], out_to.at[m], plane_out.at[m])

    def swap(m):
        return pltpu.make_async_remote_copy(
            src_ref=field_in.at[m],
            dst_ref=field.at[home, m],
            send_sem=swap_sent,
            recv_sem=swapped.at[m],
            **target(twin),
        )

    def wait_bytes(ref, sem):
        pltpu.make_async_copy(ref, ref, sem).wait()

    def send_forward(index, half, slot, start, length, near_sem):
        buffer = index % 2
        source_rows = pl.ds(pl.multiple_of(slot * block + start, 8), length)
        target_rows = pl.ds(pl.multiple_of(unit_at(slot) * block + start, 8), length)
        sent, came = sent_f.at[index, half], came_f.at[index, half]

        def single(group, to):
            return dict(
                src_ref=send_f.at[buffer, half, group // CORES, to, group % CORES, source_rows, :],
                dst_ref=got_f.at[buffer, half, 0, target_rows, :],
            )

        def double(group):
            return dict(
                src_ref=send_f.at[
                    buffer, half, group // CORES, pl.ds(1, 2), group % CORES, source_rows, :
                ],
                dst_ref=got_f.at[buffer, half, :, target_rows, :],
            )

        def away(refs, group, to, sem):
            device = (group // CORES) * columns + to * CORES + group % CORES
            pltpu.make_async_remote_copy(
                **refs, send_sem=sent, recv_sem=sem, **target(device)
            ).start()

        def own(refs):
            pltpu.make_async_copy(refs["src_ref"], refs["dst_ref"], came).start()

        @pl.when(middle)
        def _():
            own(double(my_group))
            away(single(my_group, outer), my_group, outer, came)

            def one(offset, carry):
                group = (my_group + offset) % groups
                away(single(group, outer), group, outer, came)
                away(double(group), group, layer, came)
                return carry

            lax.fori_loop(1, groups, one, 0)

        @pl.when(jnp.logical_not(middle))
        def _():
            own(single(my_group, layer))

            def one(offset, carry):
                group = (my_group + offset) % groups
                away(double(group), group, near, came_f.at[index, near_sem])
                away(single(group, LAYERS - 1 - layer), group, LAYERS - 1 - layer, came)

                @pl.when(offset > 0)
                def _():
                    away(single(group, layer), group, layer, came)

                return carry

            lax.fori_loop(0, groups, one, 0)

    def pass_forward(index, half, start, length, near_sem):
        buffer = index % 2

        @pl.when(middle)
        def _():
            wait_bytes(
                got_f.at[buffer, half, :, pl.ds(0, groups * length), :],
                came_f.at[index, near_sem],
            )

            def one(group, carry):
                unit = (group // CORES) * columns + outer * CORES + group % CORES
                region = got_f.at[
                    buffer, half, :, pl.ds(pl.multiple_of(unit * block + start, 8), length), :
                ]
                pltpu.make_async_remote_copy(
                    src_ref=region,
                    dst_ref=region,
                    send_sem=passed_f.at[index],
                    recv_sem=twin_f.at[index, half],
                    **target(twin),
                ).start()
                return carry

            lax.fori_loop(0, groups, one, 0)

    def pass_forward_part(index, part):
        pass_forward(index, 0, part * share_y, share_y, 2 + part)

    def pass_forward_chunk(index, number):
        pass_forward(index, 1, number * chunk, chunk, 2 + parts + number)

    def send_second_half(index):
        def slot_loop(slot, carry):
            def one(number, inner):
                send_forward(index, 1, slot, number * chunk, chunk, 2 + parts + number)
                return inner

            return lax.fori_loop(0, chunks, one, carry)

        lax.fori_loop(0, units, slot_loop, 0)

    def send_inverse(index, half, part):
        start = part * share_y
        sent, came = sent_i.at[index, half], came_i.at[index, part]
        mine = pl.ds(pl.multiple_of(start, 8), share_y)

        def rows_of(group, to):
            unit = (group // CORES) * columns + to * CORES + group % CORES
            return pl.ds(pl.multiple_of(unit * block + start, 8), share_y)

        def away(refs, group, to, sem):
            device = (group // CORES) * columns + to * CORES + group % CORES
            pltpu.make_async_remote_copy(
                **refs, send_sem=sent, recv_sem=sem, **target(device)
            ).start()

        def own(refs):
            pltpu.make_async_copy(refs["src_ref"], refs["dst_ref"], came).start()

        @pl.when(middle)
        def _():
            def refs(group, to, slot):
                return dict(
                    src_ref=send_i.at[half, :, rows_of(group, to), :],
                    dst_ref=got_i.at[slot, half, row, pl.ds(1, 2), core, mine, :],
                )

            for slot in range(2):
                own(refs(my_group, slot + 1, slot))
            away(refs(my_group, outer, 0), my_group, outer, came)

            def one(offset, carry):
                group = (my_group + offset) % groups
                away(refs(group, outer, 0), group, outer, came)
                for slot in range(2):
                    away(refs(group, slot + 1, slot), group, layer, came)
                return carry

            lax.fori_loop(1, groups, one, 0)

        @pl.when(jnp.logical_not(middle))
        def _():
            def refs(group, to, slot):
                return dict(
                    src_ref=send_i.at[half, 0, rows_of(group, to), :],
                    dst_ref=got_i.at[slot, half, row, layer, core, mine, :],
                )

            own(refs(my_group, layer, 0))

            def one(offset, carry):
                group = (my_group + offset) % groups
                for slot in range(2):
                    away(refs(group, slot + 1, slot), group, near, near_i.at[index, half, part])
                away(
                    refs(group, LAYERS - 1 - layer, 0), group, LAYERS - 1 - layer, came
                )

                @pl.when(offset > 0)
                def _():
                    away(refs(group, layer, 0), group, layer, came)

                return carry

            lax.fori_loop(0, groups, one, 0)

    def pass_inverse(index, half, part):
        mine = pl.ds(pl.multiple_of(part * share_y, 8), share_y)

        @pl.when(middle)
        def _():
            wait_bytes(got_i.at[:, half, :, 1, :, mine, :], near_i.at[index, half, part])

            def one(group, carry):
                region = got_i.at[:, half, group // CORES, outer, group % CORES, mine, :]
                pltpu.make_async_remote_copy(
                    src_ref=region,
                    dst_ref=region,
                    send_sem=passed_i.at[index],
                    recv_sem=twin_i.at[index, part],
                    **target(twin),
                ).start()
                return carry

            lax.fori_loop(0, groups, one, 0)

    def wait_sent(sem):
        @pl.when(middle)
        def _():
            wait_bytes(got_f.at[0, 0, :, pl.ds(0, (groups * 3 - 2) * block), :], sem)

        @pl.when(jnp.logical_not(middle))
        def _():
            wait_bytes(got_f.at[0, 0, 0, pl.ds(0, (groups * 4 - 1) * block), :], sem)

    def wait_sent_forward(index):
        for half in range(halves):
            wait_sent(sent_f.at[index, half])

    def wait_passed(sem):
        @pl.when(middle)
        def _():
            wait_bytes(got_f.at[0, 0, 0], sem)

    def plane(index, slot, m, values):
        spectrum = mul_left(mul_right(values))
        rows = pl.ds(pl.multiple_of(slot * block + m * share_y, 8), share_y)
        for half in range(halves):
            part = spectrum[:, half * LANES : (half + 1) * LANES]
            send_f[index % 2, half, :, :, :, rows, :] = part.reshape(
                count // columns, LAYERS, CORES, share_y, LANES
            )

    def send_plane(index, slot, m):
        send_forward(index, 0, slot, m * share_y, share_y, 2 + m)

    def physical(slot, m):
        rows = pl.ds(pl.multiple_of(m * share_y, 8), share_y)
        values = [
            got_i[slot, half, :, :, :, rows, :].reshape(size_y, LANES) for half in range(halves)
        ]
        return mul_right(mul_left(jnp.concatenate(values, axis=1)))

    def spectrum_at(index, half, pair):
        values = [
            got_f[
                index % 2, half, pair // pairs,
                pl.ds(pair % pairs * 2 + inner, size_x, stride=share_y), :,
            ]
            for inner in range(2)
        ]
        return mul_left(jnp.concatenate(values, axis=1))

    def arrived_forward(index, half):
        wait_bytes(got_f.at[index % 2, half, 0], came_f.at[index, half])

        @pl.when(middle)
        def _():
            wait_bytes(
                got_f.at[index % 2, half, :, pl.ds(0, groups * block), :], twin_f.at[index, half]
            )

    def arrived_inverse(index, part):
        rows = pl.ds(pl.multiple_of(part * share_y, 8), share_y)
        wait_bytes(got_i.at[0, :, :, :, :, rows, :], came_i.at[index, part])

        @pl.when(middle)
        def _():
            wait_bytes(got_i.at[:, :, :, 1, :, rows, :], twin_i.at[index, part])

    def inverse(index, sources, update):
        for half in range(halves):
            for source in sources:
                arrived_forward(source, half)
            if index > 0:
                wait_sent(sent_i.at[index - 1, half])

            def step(pair, carry):
                spectra = [spectrum_at(source, half, pair) for source in sources]
                values = mul_left(update(half, pair, *spectra))
                for inner in range(2):
                    send_i[
                        half, pair // pairs,
                        pl.ds(pair % pairs * 2 + inner, size_x, stride=share_y), :,
                    ] = values[:, inner * LANES : (inner + 1) * LANES]
                return carry

            def quarter(number, carry):
                lax.fori_loop(number * units, (number + 1) * units, step, 0)
                if half == 1:
                    pass_inverse(index, 0, number)
                elif index > 0:
                    pass_forward_chunk(sources[-1], number)
                return carry

            lax.fori_loop(0, pairs, quarter, 0)
            if half == 1:
                for source in sources:
                    wait_passed(passed_f.at[source])

            def first_parts(part, carry):
                send_inverse(index, half, part)
                return carry

            lax.fori_loop(0, early, first_parts, 0)

        def last_parts(part, carry):
            for half in range(halves):
                send_inverse(index, half, part)
            return carry

        lax.fori_loop(early, parts, last_parts, 0)
        for part in range(2):
            pass_inverse(index, 1, part)

    def pass_ahead(index, part):
        @pl.when(part + 2 < parts)
        def _():
            pass_inverse(index, 1, part + 2)

        @pl.when(jnp.logical_and(part + 2 >= early, part + 2 < parts))
        def _():
            pass_inverse(index, 0, part + 2)

    def forward(index, stage):
        def step(m, carry):
            pass_ahead(stage, m)
            arrived_inverse(stage, m)

            def one(slot, inner):
                plane(index, slot, m, reaction(physical(slot, m)))
                return inner

            lax.fori_loop(0, units, one, 0)

            @pl.when(m == parts - 1)
            def _():
                wait_passed(passed_i.at[stage])

            def send(slot, inner):
                send_plane(index, slot, m)
                return inner

            lax.fori_loop(0, units, send, 0)

            @pl.when(m >= 2)
            def _():
                pass_forward_part(index, m - 2)

            return carry

        lax.fori_loop(0, parts, step, 0)
        send_second_half(index)
        for part in range(parts - 2, parts):
            pass_forward_part(index, part)

    def wave(indices, length):
        signed = jnp.where(indices * 2 < length, indices, indices - length)
        return wave_scale * signed.astype(jnp.float32) / length

    for m in range(rows_x):
        load(m).start()
    barrier = pltpu.get_barrier_semaphore()

    def greet(offset, carry):
        pl.semaphore_signal(barrier, inc=1, **target((me + offset) % count))
        return carry

    lax.fori_loop(1, count, greet, 0)
    pl.semaphore_wait(barrier, count - 1)

    @pl.when(middle)
    def _():
        for m in range(rows_x):
            swap(m).start()

    def begin_first(m, carry):
        load(m).wait()
        plane(0, home, m, field[home, m])
        send_plane(0, home, m)
        return carry

    def begin_second(m, carry):
        plane(1, home, m, reaction(field[home, m]))
        send_plane(1, home, m)
        return carry

    lax.fori_loop(0, parts, begin_first, 0)
    lax.fori_loop(0, parts, begin_second, 0)

    @pl.when(middle)
    def _():
        other = 1 - home

        def begin_twin(m, carry):
            swap(m).wait_recv()
            plane(0, other, m, field[other, m])
            send_plane(0, other, m)
            plane(1, other, m, reaction(field[other, m]))
            send_plane(1, other, m)
            pass_forward_part(0, m)
            pass_forward_part(1, m)
            return carry

        lax.fori_loop(0, parts, begin_twin, 0)
        for m in range(rows_x):
            swap(m).wait_send()

    for index in range(2):
        send_second_half(index)

    rows_step = 32
    steps = size_x // rows_step

    def factors(item, carry):
        pair = item // steps
        start = pl.multiple_of(item % steps * rows_step, 8)
        where = pl.ds(start, rows_step)
        dims = (rows_step, 2 * LANES)
        lane = lax.broadcasted_iota(jnp.int32, dims, 1)
        second = (lane >= LANES).astype(jnp.int32)
        index_y = second + (unit_at(pair // pairs) * share_y + pair % pairs * 2)
        index_x = lax.broadcasted_iota(jnp.int32, dims, 0) + start
        wave_y, wave_x = wave(index_y, size_y), wave(index_x, size_x)
        for half in range(halves):
            wave_z = wave(lane - second * LANES + half * LANES, size_z)
            ksq = wave_y * wave_y + wave_z * wave_z + wave_x * wave_x
            values = step_factors(ksq)
            for ref, value in zip((e_half, q_half, total, held, f_two, f_three), values):
                ref[half, pair, where, :] = value
        return carry

    lax.fori_loop(0, units * pairs * steps, factors, 0)

    for index in range(2):
        for number in range(chunks):
            pass_forward_chunk(index, number)

    def update_first(half, pair, state_hat, react_u):
        base = e_half[half, pair] * state_hat
        gain = q_half[half, pair] * react_u
        first_hat = base + gain
        total[half, pair] = total[half, pair] * state_hat + held[half, pair] * react_u
        third[half, pair] = e_half[half, pair] * first_hat - gain
        held[half, pair] = base
        return first_hat

    def update_second(half, pair, react_a):
        total[half, pair] = total[half, pair] + 2.0 * f_two[half, pair] * react_a
        return held[half, pair] + q_half[half, pair] * react_a

    def update_third(half, pair, react_b):
        total[half, pair] = total[half, pair] + 2.0 * f_two[half, pair] * react_b
        return third[half, pair] + 2.0 * q_half[half, pair] * react_b

    def update_last(half, pair, react_c):
        return total[half, pair] + f_three[half, pair] * react_c

    inverse(0, (0, 1), update_first)
    for index, update in enumerate((update_second, update_third, update_last)):
        wait_sent_forward(index)
        forward(index + 2, index)
        inverse(index + 1, (index + 2,), update)
    for index in (3, 4):
        wait_sent_forward(index)

    def finish(m, carry):
        pass_ahead(3, m)
        arrived_inverse(3, m)
        field[0, m] = physical(home, m)
        store(m).start()
        return carry

    lax.fori_loop(0, parts, finish, 0)
    wait_passed(passed_i.at[3])
    for half in range(halves):
        wait_sent(sent_i.at[3, half])
    for m in range(rows_x):
        store(m).wait()


def body(initial_field):
    rows_x, size_y, size_z = initial_field.shape
    columns = lax.axis_size("col")
    rows = lax.axis_size("row")
    count = rows * columns
    size_x = rows_x * count
    share_y = size_y // count
    fits = share_y == ROWS and rows_x == ROWS and columns == LAYERS * CORES
    fits = fits and size_z == 2 * LANES and size_x == size_y == size_z
    if not fits:
        return plain_body(initial_field)
    upper, lower = split_table(size_x)
    left = np.concatenate([upper, upper, lower], axis=1)
    right = np.concatenate([upper, upper, lower], axis=0)
    halves, pairs, block = size_z // LANES, share_y // 2, rows_x * share_y
    spectral = pltpu.VMEM((halves, 2 * pairs, size_x, 2 * LANES), jnp.float32)
    vmem = pl.BlockSpec(memory_space=pltpu.VMEM)
    dma = pltpu.SemaphoreType.DMA
    return pl.pallas_call(
        functools.partial(kernel, count, columns, rows_x, share_y, size_x, size_y, size_z),
        out_shape=jax.ShapeDtypeStruct(initial_field.shape, jnp.float32),
        in_specs=[pl.BlockSpec(memory_space=pltpu.HBM), vmem, vmem],
        out_specs=pl.BlockSpec(memory_space=pltpu.HBM),
        scratch_shapes=[
            pltpu.VMEM((2, halves, rows, LAYERS, CORES, 2 * block, LANES), jnp.float32),
            pltpu.VMEM((2, halves, 2, count * block, LANES), jnp.float32),
            pltpu.VMEM((halves, 2, count * block, LANES), jnp.float32),
            pltpu.VMEM((2, halves, rows, LAYERS, CORES, block, LANES), jnp.float32),
        ]
        + [spectral] * 6
        + [
            pltpu.VMEM((2,) + initial_field.shape, jnp.float32),
            dma((5, 2 + rows_x + 4)),
            dma((5, halves)),
            dma((5, halves)),
            dma((5,)),
            dma((4, rows_x)),
            dma((4, halves, rows_x)),
            dma((4, rows_x)),
            dma((4, halves)),
            dma((4,)),
            dma((rows_x,)),
            dma,
            dma((rows_x,)),
            dma((rows_x,)),
        ],
        compiler_params=pltpu.CompilerParams(
            collective_id=0, has_side_effects=True, vmem_limit_bytes=60 * 1024 * 1024
        ),
    )(initial_field, jnp.asarray(left), jnp.asarray(right))


def solution(mesh):
    placed = (P(("row", "col"), None, None),)
    return jax.shard_map(
        body, mesh=mesh, in_specs=placed, out_specs=P(("row", "col"), None, None), check_vma=False
    )
```
